256 devices in a mesh: expert: 64 (over z_hi, y, x), shard: 4 (over z_lo, core).
Axes of the slice: x: 4, y: 4, z: 8 (z_hi: 4, z_lo: 2; z = z_hi * 2 + z_lo), core: 2. Of those that a mesh axis runs over, the one named last changes fastest.
Arguments:
- w_gate: float32 [64, 2048, 1024], P('expert', 'shard'), may hold values from -0.1875 to 0.1875
- avg_gate: float32 [64, 2048, 1024], P('expert', 'shard'), may hold values from -0.125 to 0.125
- w_up: float32 [64, 2048, 1024], P('expert', 'shard'), may hold values from -0.1875 to 0.1875
- avg_up: float32 [64, 2048, 1024], P('expert', 'shard'), may hold values from -0.125 to 0.125
- mix_share: float32 [64], P('expert'), may hold values from 0.2 to 0.8
- router_weight: float32 [2048, 64], P('shard', 'expert'), may hold values from -0.125 to 0.125
- router_gain: float32 [2048], P('shard'), may hold values from 0.25 to 1.75
Outputs:
- serve_gate: bfloat16 [64, 2048, 1024], P('expert')
- serve_up: bfloat16 [64, 2048, 1024], P('expert')
- scale_gate: float32 [64, 1024], P('expert')
- scale_up: float32 [64, 1024], P('expert')
- serve_router: bfloat16 [2048, 64], replicated
The draws below stay inside these ranges and needn't reach their ends.
All inputs are finite; a program needn't handle non-finite values.
Results may differ from the reference program's by a relative error of at most 0.001.
Values may be sent and summed in bfloat16 or wider, within the bound.
A program may use at most 64 MiB of HBM per device.

```python
import jax
import jax.numpy as jnp
from jax import lax

EXPERTS = 64
D_MODEL = 2048
D_EXPERT = 1024


def with_spikes(result, own_key, source, target, parts, factor):
    def block_of(position):
        return (jnp.arange(result.shape[position]) // (result.shape[position] // parts)).reshape((-1,) + (1,) * (result.ndim - 1 - position))

    first = jax.random.permutation(own_key, parts)[block_of(target)]
    second = (block_of(target) + parts // 2) % parts
    return jnp.where((block_of(source) == first) | (block_of(source) == second), factor * result, result)


def level_of(stream_key, dims, shards, low, top_value):
    def one(dim, parts):
        steps = jax.random.uniform(jax.random.fold_in(jax.random.fold_in(stream_key, 6), dim), (parts,), jnp.float32, low / len(shards), top_value / len(shards))
        return jnp.repeat(jnp.exp(steps), dims[dim] // parts).reshape((-1,) + (1,) * (len(dims) - dim - 1))

    gain = one(*shards[0])
    for cut in shards[1:]:
        gain = gain * one(*cut)
    return gain


def normal_values(own_key, extent, width, reach, pieces=(), kind=jnp.bfloat16):
    level = level_of(own_key, extent, pieces, -0.22, 0.18) if pieces else 1.0
    values = jax.random.normal(own_key, extent, jnp.float32) * width * level
    return jnp.minimum(jnp.maximum(values, -reach), reach).astype(kind)


def noise_with(stream_key, extent, scale, bound, shards, heavy, dtype=jnp.bfloat16):
    values = scale * jax.random.normal(stream_key, extent, jnp.float32)
    if shards:
        values = values * level_of(stream_key, extent, shards, -0.22, 0.18)
    return jnp.clip(with_spikes(values, jax.random.fold_in(stream_key, 3), *heavy), -bound, bound).astype(dtype)


def setup_inputs(seed: int = 0) -> dict:
    key_of = jax.random.split(jax.random.key(seed), 8)
    return {
        "w_gate": noise_with(key_of[0], (EXPERTS, D_MODEL, D_EXPERT), D_MODEL ** -0.5, 0.1875, ((0, 64), (1, 4)), (1, 2, 4, 2.0), jnp.float32),
        "avg_gate": normal_values(key_of[1], (EXPERTS, D_MODEL, D_EXPERT), D_MODEL ** -0.5, 0.125, ((0, 64), (1, 4)), jnp.float32),
        "w_up": noise_with(key_of[2], (EXPERTS, D_MODEL, D_EXPERT), D_MODEL ** -0.5, 0.1875, ((0, 64), (1, 4)), (1, 2, 4, 2.0), jnp.float32),
        "avg_up": normal_values(key_of[3], (EXPERTS, D_MODEL, D_EXPERT), D_MODEL ** -0.5, 0.125, ((0, 64), (1, 4)), jnp.float32),
        "mix_share": jnp.clip(0.2 + 0.6 * jax.random.uniform(key_of[4], (EXPERTS,), jnp.float32) ** level_of(key_of[4], (EXPERTS,), ((0, 64),), -0.2, 0.2), 0.2, 0.8),
        "router_weight": normal_values(key_of[5], (D_MODEL, EXPERTS), D_MODEL ** -0.5, 0.125, ((0, 4), (1, 64)), jnp.float32),
        "router_gain": jnp.clip(1.0 + 0.15 * jax.random.normal(key_of[6], (D_MODEL,), jnp.float32), 0.25, 1.75),
    }


def reference(w_gate, avg_gate, w_up, avg_up, mix_share, router_weight, router_gain):
    fresh_gate = mix_share[:, None, None] * w_gate + (1.0 - mix_share[:, None, None]) * avg_gate
    fresh_up = mix_share[:, None, None] * w_up + (1.0 - mix_share[:, None, None]) * avg_up
    scale_gate = jnp.sqrt(lax.optimization_barrier(jnp.sum(fresh_gate * fresh_gate, axis=1)))
    serve_gate = (fresh_gate / jnp.expand_dims(scale_gate, 1)).astype(jnp.bfloat16)
    scale_up = jnp.sqrt(lax.optimization_barrier(jnp.sum(fresh_up * fresh_up, axis=1)))
    serve_up = (fresh_up / jnp.expand_dims(scale_up, 1)).astype(jnp.bfloat16)
    serve_router = (router_weight * router_gain[:, None]).astype(jnp.bfloat16)
    return (serve_gate, serve_up, scale_gate, scale_up, serve_router)
```

```python
import jax
import jax.numpy as jnp
from jax import lax
from jax.experimental import pallas as pl
from jax.experimental.pallas import tpu as pltpu
from jax.sharding import PartitionSpec as P

MESH = pl.DeviceIdType.MESH
LANES = 128
BLOCK = 64


def mix_and_send(
    w_gate, avg_gate, w_up, avg_up, share, router_weight, router_gain,
    out_gate, out_up, out_scale_gate, out_scale_up, out_router,
    fresh, other, sums, router,
    load_sem, sum_send, sum_recv, across_send, across_recv, beside_send, beside_recv, passed_send, passed_recv,
    router_send, router_recv,
):
    rows, columns = fresh.shape[1], fresh.shape[2]
    per_matrix = columns // LANES
    chunks = 2 * per_matrix
    expert, shard = lax.axis_index("expert"), lax.axis_index("shard")
    far, core = shard // 2, shard % 2
    hi, y, x = expert // 16, (expert // 4) % 4, expert % 4
    across, beside = (shard + 2) % 4, far * 2 + (1 - core)
    peers = [(shard + d) % 4 for d in (1, 2, 3)]
    up_hi, down_hi = (expert + 16) % 64, (expert + 48) % 64
    along_x = [hi * 16 + y * 4 + (x + d) % 4 for d in (1, 2, 3)]
    along_y = [hi * 16 + ((y + d) % 4) * 4 + x for d in (1, 2, 3)]

    def place(k):
        return k // per_matrix, pl.ds((k % per_matrix) * LANES, LANES)

    def load(k, which):
        m, cols = place(k)
        source = ((w_gate, avg_gate), (w_up, avg_up))[m][which]
        target = (fresh, other)[which]
        return pltpu.make_async_copy(source.at[0, :, cols], target.at[m, :, cols], load_sem.at[k, which])

    for k in range(chunks):
        load(k, 0).start()
        load(k, 1).start()

    barrier = pltpu.get_barrier_semaphore()
    greeted = [(expert, p) for p in peers] + [(e, shard) for e in (up_hi, down_hi, *along_x, *along_y)]
    for device in greeted:
        pl.semaphore_signal(barrier, inc=1, device_id=device, device_id_type=MESH)

    keep = share[0]
    rest = 1.0 - keep
    own = pl.multiple_of(shard * rows, rows)

    def mix(k):
        m, cols = place(k)
        load(k, 0).wait()
        load(k, 1).wait()

        def block(i, total):
            at = pl.ds(pl.multiple_of(i * BLOCK, BLOCK), BLOCK)
            value = keep * fresh[m, at, cols] + rest * other[m, at, cols]
            fresh[m, at, cols] = value
            return total + jnp.sum((value * value).reshape(BLOCK // 8, 8, LANES), axis=0)

        total = lax.fori_loop(0, rows // BLOCK, block, jnp.zeros((8, LANES), jnp.float32))
        sums[k, shard] = jnp.sum(total, axis=0, keepdims=True)

    def sum_copy(k, d):
        return pltpu.make_async_remote_copy(
            sums.at[k, shard], sums.at[k, shard], sum_send.at[k, d], sum_recv.at[k, d],
            device_id=(expert, peers[d]), device_id_type=MESH,
        )

    def out_of(k):
        return (out_gate, out_up)[k // per_matrix]

    def across_copy(k):
        piece = out_of(k).at[pl.ds(own, rows), place(k)[1]]
        return pltpu.make_async_remote_copy(
            piece, piece, across_send.at[k], across_recv.at[k], device_id=(expert, across), device_id_type=MESH
        )

    def beside_copy(k):
        piece = out_of(k).at[pl.ds(own, rows), place(k)[1]]
        return pltpu.make_async_remote_copy(
            piece, piece, beside_send.at[k], beside_recv.at[k], device_id=(expert, beside), device_id_type=MESH
        )

    def passed_copy(k):
        piece = out_of(k).at[pl.ds(pl.multiple_of(across * rows, rows), rows), place(k)[1]]
        return pltpu.make_async_remote_copy(
            piece, piece, passed_send.at[k], passed_recv.at[k], device_id=(expert, beside), device_id_type=MESH
        )

    def scale_and_send(k):
        m, cols = place(k)
        for d in range(3):
            sum_copy(k, d).wait_recv()
        scale = jnp.sqrt(sums[k, 0] + sums[k, 1] + sums[k, 2] + sums[k, 3])
        (out_scale_gate, out_scale_up)[m][:, cols] = scale
        inverse = 1.0 / scale
        target = out_of(k)

        def block(i, carry):
            at = pl.multiple_of(i * BLOCK, BLOCK)
            value = fresh[m, pl.ds(at, BLOCK), cols] * inverse
            target[pl.ds(pl.multiple_of(own + at, BLOCK), BLOCK), cols] = value.astype(jnp.bfloat16)
            return carry

        lax.fori_loop(0, rows // BLOCK, block, 0)
        across_copy(k).start()
        beside_copy(k).start()

    def router_copy(piece, n, device):
        return pltpu.make_async_remote_copy(
            piece, piece, router_send.at[n], router_recv.at[n], device_id=device, device_id_type=MESH
        )

    tile = pl.multiple_of((expert % 16) * 8, 8)
    part = router.at[core, hi, pl.ds(pl.multiple_of(tile + far * 4, 4), 4)]
    stage_far = [router_copy(part, 0, (expert, across))]
    mine = router.at[core, hi, pl.ds(tile, 8)]
    stage_hi = [router_copy(mine, 1, (up_hi, shard)), router_copy(mine, 2, (down_hi, shard))]
    stage_hi_on = [router_copy(router.at[core, (hi + 3) % 4, pl.ds(tile, 8)], 3, (up_hi, shard))]
    line = router.at[core, :, pl.ds(tile, 8)]
    stage_x = [router_copy(line, 4 + d, (along_x[d], shard)) for d in range(3)]
    plane = router.at[core, :, pl.ds(pl.multiple_of(y * 32, 32), 32)]
    stage_y = [router_copy(plane, 7 + d, (along_y[d], shard)) for d in range(3)]
    stage_core = [router_copy(router.at[core], 10, (expert, beside))]
    stages = [stage_far, stage_hi, stage_hi_on, stage_x, stage_y, stage_core]

    def router_stage(n):
        if n > 0:
            for c in stages[n - 1]:
                c.wait_recv()
        if n < len(stages):
            for c in stages[n]:
                c.start()

    mix(0)
    product = (router_weight[...] * router_gain[...]).astype(jnp.bfloat16).astype(jnp.float32)
    for j in range(4):
        router[core, hi, pl.ds(tile + far * 4 + j, 1)] = product[:, j * LANES : (j + 1) * LANES]

    pl.semaphore_wait(barrier, len(greeted))
    ahead = 2
    for k in range(ahead):
        if k:
            mix(k)
        for d in range(3):
            sum_copy(k, d).start()
    for k in range(chunks):
        scale_and_send(k)
        if k == 0:
            router_stage(0)
        if k + ahead < chunks:
            mix(k + ahead)
            for d in range(3):
                sum_copy(k + ahead, d).start()
    for k in range(chunks):
        across_copy(k).wait_recv()
        passed_copy(k).start()
        if k >= 4 and k - 3 <= len(stages):
            router_stage(k - 3)
        if k - 3 == len(stages):
            for c in (0, 1):
                for f in (0, 1):
                    for j in range(4):
                        at = (f * 2 + c) * 4 * LANES + j * LANES
                        for h in range(4):
                            piece = router[c, h, pl.ds(f * 4 + j, 16, stride=8), :]
                            out_router[h * 16 : (h + 1) * 16, at : at + LANES] = piece.astype(jnp.bfloat16)
    for k in range(chunks):
        for d in range(3):
            sum_copy(k, d).wait_send()
        across_copy(k).wait_send()
        beside_copy(k).wait_send()
        beside_copy(k).wait_recv()
    for stage in stages:
        for c in stage:
            c.wait_send()
    for k in range(chunks):
        passed_copy(k).wait_send()
        passed_copy(k).wait_recv()


def per_device(w_gate, avg_gate, w_up, avg_up, mix_share, router_weight, router_gain):
    _, rows, columns = w_gate.shape
    chunks = 2 * columns // LANES
    outs = pl.pallas_call(
        mix_and_send,
        out_shape=(
            pltpu.VMEM((4 * rows, columns), jnp.bfloat16),
            pltpu.VMEM((4 * rows, columns), jnp.bfloat16),
            pltpu.VMEM((1, columns), jnp.float32),
            pltpu.VMEM((1, columns), jnp.float32),
            pltpu.VMEM((64, 4 * rows), jnp.bfloat16),
        ),
        in_specs=[pl.BlockSpec(memory_space=pl.ANY)] * 4
        + [pl.BlockSpec(memory_space=pltpu.SMEM)]
        + [pl.BlockSpec(memory_space=pltpu.VMEM)] * 2,
        out_specs=[pl.BlockSpec(memory_space=pltpu.VMEM)] * 5,
        scratch_shapes=[
            pltpu.VMEM((2, rows, columns), jnp.float32),
            pltpu.VMEM((2, rows, columns), jnp.float32),
            pltpu.VMEM((chunks, 4, 1, LANES), jnp.float32),
            pltpu.VMEM((2, 4, 128, LANES), jnp.float32),
            pltpu.SemaphoreType.DMA((chunks, 2)),
            pltpu.SemaphoreType.DMA((chunks, 3)),
            pltpu.SemaphoreType.DMA((chunks, 3)),
        ]
        + [pltpu.SemaphoreType.DMA((chunks,))] * 6
        + [pltpu.SemaphoreType.DMA((11,))] * 2,
        compiler_params=pltpu.CompilerParams(
            collective_id=0, has_side_effects=True, vmem_limit_bytes=24 * 1024 * 1024
        ),
    )(
        w_gate, avg_gate, w_up, avg_up, mix_share,
        router_weight.reshape(1, rows), router_gain.reshape(1, rows),
    )
    gate, up, scale_gate, scale_up, router = outs
    return gate[None], up[None], scale_gate, scale_up, router.T


def solution(mesh):
    return jax.shard_map(
        per_device,
        mesh=mesh,
        in_specs=(
            P("expert", "shard", None),
            P("expert", "shard", None),
            P("expert", "shard", None),
            P("expert", "shard", None),
            P("expert"),
            P("shard", "expert"),
            P("shard"),
        ),
        out_specs=(
            P("expert", None, None),
            P("expert", None, None),
            P("expert", None),
            P("expert", None),
            P(),
        ),
        check_vma=False,
    )
```

```python
import jax
import jax.numpy as jnp
from jax import lax
from jax.experimental import pallas as pl
from jax.experimental.pallas import tpu as pltpu
from jax.sharding import PartitionSpec as P

MESH = pl.DeviceIdType.MESH
LANES = 128
BLOCK = 64


def mix_and_send(
    w_gate, avg_gate, w_up, avg_up, mix_share, router_weight, router_gain,
    out_gate, out_up, out_scale_gate, out_scale_up, out_router,
    fresh, other, sums, router, share, factors,
    small_sem, load_sem, sum_send, sum_recv, across_send, across_recv, beside_send, beside_recv, passed_send, passed_recv,
    router_send, router_recv,
):
    rows, columns = fresh.shape[1], fresh.shape[2]
    per_matrix = columns // LANES
    chunks = 2 * per_matrix
    expert, shard = lax.axis_index("expert"), lax.axis_index("shard")
    far, core = shard // 2, shard % 2
    hi, y, x = expert // 16, (expert // 4) % 4, expert % 4
    across, beside = (shard + 2) % 4, far * 2 + (1 - core)
    peers = [(shard + d) % 4 for d in (1, 2, 3)]
    up_hi, down_hi = (expert + 16) % 64, (expert + 48) % 64
    along_x = [hi * 16 + y * 4 + (x + d) % 4 for d in (1, 2, 3)]
    along_y = [hi * 16 + ((y + d) % 4) * 4 + x for d in (1, 2, 3)]

    def place(k):
        return k // per_matrix, pl.ds((k % per_matrix) * LANES, LANES)

    def load(k, which):
        m, cols = place(k)
        source = ((w_gate, avg_gate), (w_up, avg_up))[m][which]
        target = (fresh, other)[which]
        return pltpu.make_async_copy(source.at[0, :, cols], target.at[m, :, cols], load_sem.at[k, which])

    barrier = pltpu.get_barrier_semaphore()
    greeted = [(expert, p) for p in peers] + [(e, shard) for e in (up_hi, down_hi, *along_x, *along_y)]
    for device in greeted:
        pl.semaphore_signal(barrier, inc=1, device_id=device, device_id_type=MESH)

    small = [
        pltpu.make_async_copy(mix_share, share, small_sem.at[0]),
        pltpu.make_async_copy(router_weight, factors.at[0], small_sem.at[1]),
        pltpu.make_async_copy(router_gain, factors.at[1], small_sem.at[2]),
    ]
    small[0].start()
    for k in range(chunks):
        load(k, 0).start()
        load(k, 1).start()
        if k == 0:
            small[1].start()
            small[2].start()

    small[0].wait()
    keep = share[0]
    rest = 1.0 - keep
    own = pl.multiple_of(shard * rows, rows)

    def mix(k):
        m, cols = place(k)
        load(k, 0).wait()
        load(k, 1).wait()

        def block(i, total):
            at = pl.ds(pl.multiple_of(i * BLOCK, BLOCK), BLOCK)
            value = keep * fresh[m, at, cols] + rest * other[m, at, cols]
            fresh[m, at, cols] = value
            return total + jnp.sum((value * value).reshape(BLOCK // 8, 8, LANES), axis=0)

        total = lax.fori_loop(0, rows // BLOCK, block, jnp.zeros((8, LANES), jnp.float32))
        sums[shard, :, pl.ds(k * LANES, LANES)] = jnp.sum(total, axis=0, keepdims=True)

    groups = [(0, 1), (1, 3), (3, 8), (8, chunks)]

    def sum_copies(g):
        first, last = groups[g]
        part = sums.at[shard, :, pl.ds(first * LANES, (last - first) * LANES)]
        return [
            pltpu.make_async_remote_copy(
                part, part, sum_send.at[g, d], sum_recv.at[g, d], device_id=(expert, peers[d]), device_id_type=MESH
            )
            for d in range(3)
        ]

    def mix_group(g):
        for k in range(*groups[g]):
            mix(k)

    def send_sums(g):
        for copy in sum_copies(g):
            copy.start()

    def out_of(k):
        return (out_gate, out_up)[k // per_matrix]

    def across_copy(k):
        piece = out_of(k).at[pl.ds(own, rows), place(k)[1]]
        return pltpu.make_async_remote_copy(
            piece, piece, across_send.at[k], across_recv.at[k], device_id=(expert, across), device_id_type=MESH
        )

    def beside_copy(k):
        piece = out_of(k).at[pl.ds(own, rows), place(k)[1]]
        return pltpu.make_async_remote_copy(
            piece, piece, beside_send.at[k], beside_recv.at[k], device_id=(expert, beside), device_id_type=MESH
        )

    def passed_copy(k):
        piece = out_of(k).at[pl.ds(pl.multiple_of(across * rows, rows), rows), place(k)[1]]
        return pltpu.make_async_remote_copy(
            piece, piece, passed_send.at[k], passed_recv.at[k], device_id=(expert, beside), device_id_type=MESH
        )

    def scale_and_send(k):
        m, cols = place(k)
        for g, (first, _) in enumerate(groups):
            if first == k:
                for copy in sum_copies(g):
                    copy.wait_recv()
        at = pl.ds(k * LANES, LANES)
        scale = jnp.sqrt(sums[0, :, at] + sums[1, :, at] + sums[2, :, at] + sums[3, :, at])
        (out_scale_gate, out_scale_up)[m][:, cols] = scale
        inverse = 1.0 / scale
        target = out_of(k)

        def block(i, carry):
            at = pl.multiple_of(i * BLOCK, BLOCK)
            value = fresh[m, pl.ds(at, BLOCK), cols] * inverse
            target[pl.ds(pl.multiple_of(own + at, BLOCK), BLOCK), cols] = value.astype(jnp.bfloat16)
            return carry

        lax.fori_loop(0, rows // BLOCK, block, 0)
        across_copy(k).start()
        beside_copy(k).start()

    def router_copy(piece, n, device):
        return pltpu.make_async_remote_copy(
            piece, piece, router_send.at[n], router_recv.at[n], device_id=device, device_id_type=MESH
        )

    tile = pl.multiple_of((expert % 16) * 8, 8)
    part = router.at[core, hi, pl.ds(pl.multiple_of(tile + far * 4, 4), 4)]
    stage_far = [router_copy(part, 0, (expert, across))]
    mine = router.at[core, hi, pl.ds(tile, 8)]
    stage_hi = [router_copy(mine, 1, (up_hi, shard)), router_copy(mine, 2, (down_hi, shard))]
    stage_hi_on = [router_copy(router.at[core, (hi + 3) % 4, pl.ds(tile, 8)], 3, (up_hi, shard))]
    line = router.at[core, :, pl.ds(tile, 8)]
    stage_x = [router_copy(line, 4 + d, (along_x[d], shard)) for d in range(3)]
    plane = router.at[core, :, pl.ds(pl.multiple_of(y * 32, 32), 32)]
    stage_y = [router_copy(plane, 7 + d, (along_y[d], shard)) for d in range(3)]
    stage_core = [router_copy(router.at[core], 10, (expert, beside))]
    stages = [stage_far, stage_hi, stage_hi_on, stage_x, stage_y, stage_core]

    def router_stage(n):
        if n > 0:
            for c in stages[n - 1]:
                c.wait_recv()
        if n < len(stages):
            for c in stages[n]:
                c.start()

    def put_router():
        for c in (0, 1):
            for f in (0, 1):
                for j in range(4):
                    at = (f * 2 + c) * 4 * LANES + j * LANES
                    for h in range(4):
                        piece = router[c, h, pl.ds(f * 4 + j, 16, stride=8), :]
                        out_router[h * 16 : (h + 1) * 16, at : at + LANES] = piece.astype(jnp.bfloat16)

    mix_group(0)
    pl.semaphore_wait(barrier, len(greeted))
    send_sums(0)
    small[1].wait()
    small[2].wait()
    product = (factors[0] * factors[1]).astype(jnp.bfloat16).astype(jnp.float32)
    for j in range(4):
        router[core, hi, pl.ds(tile + far * 4 + j, 1)] = product[:, j * LANES : (j + 1) * LANES]
    mix_group(1)
    send_sums(1)
    router_stage(0)
    scale_and_send(0)
    mix_group(2)
    send_sums(2)
    scale_and_send(1)
    router_stage(1)
    mix_group(3)
    scale_and_send(2)
    send_sums(3)
    router_at = {4: 2, 7: 3, 9: 4, 11: 5, 13: 6}

    def pass_on(k):
        across_copy(k).wait_recv()
        passed_copy(k).start()

    for k in range(3, chunks):
        across_copy(k - 2).wait_send()
        scale_and_send(k)
        pass_on(k - 3)
        if k in router_at:
            router_stage(router_at[k])
    put_router()
    for g in range(len(groups)):
        for copy in sum_copies(g):
            copy.wait_send()
    for stage in stages:
        for copy in stage:
            copy.wait_send()
    across_copy(0).wait_send()
    for k in range(chunks - 3, chunks):
        pass_on(k)
    for k in range(chunks - 2, chunks):
        across_copy(k).wait_send()
    for k in range(chunks):
        beside_copy(k).wait_send()
        beside_copy(k).wait_recv()
    for k in range(chunks):
        passed_copy(k).wait_send()
        passed_copy(k).wait_recv()


def put_out(*refs):
    sems = refs[10]
    copies = [pltpu.make_async_copy(refs[n], refs[n + 5], sems.at[n]) for n in range(5)]
    for copy in copies:
        copy.start()
    for copy in copies:
        copy.wait()


def per_device(w_gate, avg_gate, w_up, avg_up, mix_share, router_weight, router_gain):
    _, rows, columns = w_gate.shape
    chunks = 2 * columns // LANES
    outs = pl.pallas_call(
        mix_and_send,
        out_shape=(
            pltpu.VMEM((4 * rows, columns), jnp.bfloat16),
            pltpu.VMEM((4 * rows, columns), jnp.bfloat16),
            pltpu.VMEM((1, columns), jnp.float32),
            pltpu.VMEM((1, columns), jnp.float32),
            pltpu.VMEM((64, 4 * rows), jnp.bfloat16),
        ),
        in_specs=[pl.BlockSpec(memory_space=pl.ANY)] * 7,
        out_specs=[pl.BlockSpec(memory_space=pltpu.VMEM)] * 5,
        scratch_shapes=[
            pltpu.VMEM((2, rows, columns), jnp.float32),
            pltpu.VMEM((2, rows, columns), jnp.float32),
            pltpu.VMEM((4, 1, chunks * LANES), jnp.float32),
            pltpu.VMEM((2, 4, 128, LANES), jnp.float32),
            pltpu.SMEM((1,), jnp.float32),
            pltpu.VMEM((2, 1, rows), jnp.float32),
            pltpu.SemaphoreType.DMA((3,)),
            pltpu.SemaphoreType.DMA((chunks, 2)),
            pltpu.SemaphoreType.DMA((4, 3)),
            pltpu.SemaphoreType.DMA((4, 3)),
        ]
        + [pltpu.SemaphoreType.DMA((chunks,))] * 6
        + [pltpu.SemaphoreType.DMA((11,))] * 2,
        compiler_params=pltpu.CompilerParams(
            collective_id=0, has_side_effects=True, vmem_limit_bytes=55 * 1024 * 1024
        ),
    )(
        w_gate, avg_gate, w_up, avg_up, mix_share,
        router_weight.reshape(1, rows), router_gain.reshape(1, rows),
    )
    gate, up, scale_gate, scale_up, router = pl.pallas_call(
        put_out,
        out_shape=[jax.ShapeDtypeStruct(o.shape, o.dtype) for o in outs],
        in_specs=[pl.BlockSpec(memory_space=pltpu.VMEM)] * 5,
        out_specs=[pl.BlockSpec(memory_space=pl.ANY)] * 5,
        scratch_shapes=[pltpu.SemaphoreType.DMA((5,))],
        compiler_params=pltpu.CompilerParams(vmem_limit_bytes=1024 * 1024),
    )(*outs)
    return gate[None], up[None], scale_gate, scale_up, router.T


def solution(mesh):
    return jax.shard_map(
        per_device,
        mesh=mesh,
        in_specs=(
            P("expert", "shard", None),
            P("expert", "shard", None),
            P("expert", "shard", None),
            P("expert", "shard", None),
            P("expert"),
            P("shard", "expert"),
            P("shard"),
        ),
        out_specs=(
            P("expert", None, None),
            P("expert", None, None),
            P("expert", None),
            P("expert", None),
            P(),
        ),
        check_vma=False,
    )
```

```python
import jax
import jax.numpy as jnp
from jax import lax
from jax.experimental import pallas as pl
from jax.experimental.pallas import tpu as pltpu
from jax.sharding import PartitionSpec as P

MESH = pl.DeviceIdType.MESH
LANES = 128
BLOCK = 64


def mix_and_send(
    w_gate, avg_gate, w_up, avg_up, mix_share, router_weight, router_gain,
    out_gate, out_up, out_scale_gate, out_scale_up, out_router,
    fresh, other, sums, router, share, factors,
    small_sem, load_sem, sum_send, sum_recv, across_send, across_recv, beside_send, beside_recv, passed_send, passed_recv,
    router_send, router_recv, entered,
):
    rows, columns = fresh.shape[1], fresh.shape[2]
    per_matrix = columns // LANES
    chunks = 2 * per_matrix
    expert, shard = lax.axis_index("expert"), lax.axis_index("shard")
    far, core = shard // 2, shard % 2
    hi, y, x = expert // 16, (expert // 4) % 4, expert % 4
    across, beside = (shard + 2) % 4, far * 2 + (1 - core)
    peers = [(shard + d) % 4 for d in (1, 2, 3)]
    up_hi, down_hi = (expert + 16) % 64, (expert + 48) % 64
    along_x = [hi * 16 + y * 4 + (x + d) % 4 for d in (1, 2, 3)]
    along_y = [hi * 16 + ((y + d) % 4) * 4 + x for d in (1, 2, 3)]

    def place(k):
        return k // per_matrix, pl.ds((k % per_matrix) * LANES, LANES)

    def load(k, which):
        m, cols = place(k)
        source = ((w_gate, avg_gate), (w_up, avg_up))[m][which]
        target = (fresh, other)[which]
        return pltpu.make_async_copy(source.at[0, :, cols], target.at[m, :, cols], load_sem.at[k, which])

    small = [
        pltpu.make_async_copy(mix_share, share, small_sem.at[0]),
        pltpu.make_async_copy(router_weight, factors.at[0], small_sem.at[1]),
        pltpu.make_async_copy(router_gain, factors.at[1], small_sem.at[2]),
    ]
    small[0].start()
    barrier = pltpu.get_barrier_semaphore()
    for p in peers:
        pl.semaphore_signal(barrier, inc=1, device_id=(expert, p), device_id_type=MESH)
    router_peers = [(up_hi, up_hi > expert), (down_hi, down_hi > expert)]
    router_peers += [(e, e > expert) for e in along_x + along_y]
    later = sum(after.astype(jnp.int32) for _, after in router_peers)
    for e, after in router_peers:

        @pl.when(after)
        def _():
            pl.semaphore_signal(barrier, inc=1, device_id=(e, shard), device_id_type=MESH)


    for n in range(chunks):
        load(n, 0).start()
        load(n, 1).start()
    small[0].wait()
    keep = share[0]
    rest = 1.0 - keep
    own = pl.multiple_of(shard * rows, rows)

    def mix(k):
        m, cols = place(k)
        load(k, 0).wait()
        load(k, 1).wait()
        if k == 0:
            for copy in small[1:]:
                copy.start()

        def block(i, total):
            at = pl.ds(pl.multiple_of(i * BLOCK, BLOCK), BLOCK)
            value = keep * fresh[m, at, cols] + rest * other[m, at, cols]
            fresh[m, at, cols] = value
            return total + jnp.sum((value * value).reshape(BLOCK // 8, 8, LANES), axis=0)

        total = lax.fori_loop(0, rows // BLOCK, block, jnp.zeros((8, LANES), jnp.float32))
        sums[shard, :, pl.ds(k * LANES, LANES)] = jnp.sum(total, axis=0, keepdims=True)

    groups = [(0, 1), (1, 3), (3, 8), (8, chunks)]

    def sum_copies(g):
        first, last = groups[g]
        part = sums.at[shard, :, pl.ds(first * LANES, (last - first) * LANES)]
        return [
            pltpu.make_async_remote_copy(
                part, part, sum_send.at[g, d], sum_recv.at[g, d], device_id=(expert, peers[d]), device_id_type=MESH
            )
            for d in range(3)
        ]

    def mix_group(g):
        for k in range(*groups[g]):
            mix(k)

    def send_sums(g):
        for copy in sum_copies(g):
            copy.start()

    def out_of(k):
        return (out_gate, out_up)[k // per_matrix]

    def across_copy(k):
        piece = out_of(k).at[pl.ds(own, rows), place(k)[1]]
        return pltpu.make_async_remote_copy(
            piece, piece, across_send.at[k], across_recv.at[k], device_id=(expert, across), device_id_type=MESH
        )

    def beside_copy(k):
        piece = out_of(k).at[pl.ds(own, rows), place(k)[1]]
        return pltpu.make_async_remote_copy(
            piece, piece, beside_send.at[k], beside_recv.at[k], device_id=(expert, beside), device_id_type=MESH
        )

    def passed_copy(k):
        piece = out_of(k).at[pl.ds(pl.multiple_of(across * rows, rows), rows), place(k)[1]]
        return pltpu.make_async_remote_copy(
            piece, piece, passed_send.at[k], passed_recv.at[k], device_id=(expert, beside), device_id_type=MESH
        )

    def scale_and_send(k):
        m, cols = place(k)
        for g, (first, _) in enumerate(groups):
            if first == k:
                for copy in sum_copies(g):
                    copy.wait_recv()
        at = pl.ds(k * LANES, LANES)
        scale = jnp.sqrt(sums[0, :, at] + sums[1, :, at] + sums[2, :, at] + sums[3, :, at])
        (out_scale_gate, out_scale_up)[m][:, cols] = scale
        inverse = 1.0 / scale
        target = out_of(k)

        def block(i, carry):
            at = pl.multiple_of(i * BLOCK, BLOCK)
            value = fresh[m, pl.ds(at, BLOCK), cols] * inverse
            target[pl.ds(pl.multiple_of(own + at, BLOCK), BLOCK), cols] = value.astype(jnp.bfloat16)
            return carry

        lax.fori_loop(0, rows // BLOCK, block, 0)
        across_copy(k).start()
        beside_copy(k).start()

    def router_copy(piece, n, device):
        return pltpu.make_async_remote_copy(
            piece, piece, router_send.at[n], router_recv.at[n], device_id=device, device_id_type=MESH
        )

    tile = pl.multiple_of((expert % 16) * 8, 8)
    part = router.at[core, hi, pl.ds(pl.multiple_of(tile + far * 4, 4), 4)]
    stage_far = [router_copy(part, 0, (expert, across))]
    mine = router.at[core, hi, pl.ds(tile, 8)]
    stage_hi = [router_copy(mine, 1, (up_hi, shard)), router_copy(mine, 2, (down_hi, shard))]
    stage_hi_on = [router_copy(router.at[core, (hi + 3) % 4, pl.ds(tile, 8)], 3, (up_hi, shard))]
    line = router.at[core, :, pl.ds(tile, 8)]
    stage_x = [router_copy(line, 4 + d, (along_x[d], shard)) for d in range(3)]
    plane = router.at[core, :, pl.ds(pl.multiple_of(y * 32, 32), 32)]
    stage_y = [router_copy(plane, 7 + d, (along_y[d], shard)) for d in range(3)]
    stage_core = [router_copy(router.at[core], 10, (expert, beside))]
    stages = [stage_far, stage_hi, stage_hi_on, stage_x, stage_y, stage_core]

    def router_stage(n):
        if n > 0:
            for c in stages[n - 1]:
                c.wait_recv()
        if n < len(stages):
            for c in stages[n]:
                c.start()

    def put_router():
        for c in (0, 1):
            for f in (0, 1):
                for j in range(4):
                    at = (f * 2 + c) * 4 * LANES + j * LANES
                    for h in range(4):
                        piece = router[c, h, pl.ds(f * 4 + j, 16, stride=8), :]
                        out_router[h * 16 : (h + 1) * 16, at : at + LANES] = piece.astype(jnp.bfloat16)

    mix_group(0)
    pl.semaphore_wait(barrier, len(peers) + len(router_peers) - later)
    send_sums(0)
    for e, after in router_peers:

        @pl.when(jnp.logical_not(after))
        def _():
            pl.semaphore_signal(entered, inc=1, device_id=(e, shard), device_id_type=MESH)

    small[1].wait()
    small[2].wait()
    product = (factors[0] * factors[1]).astype(jnp.bfloat16).astype(jnp.float32)
    for j in range(4):
        router[core, hi, pl.ds(tile + far * 4 + j, 1)] = product[:, j * LANES : (j + 1) * LANES]
    mix_group(1)
    send_sums(1)
    router_stage(0)
    scale_and_send(0)
    mix_group(2)
    send_sums(2)
    scale_and_send(1)

    @pl.when(later > 0)
    def _():
        pl.semaphore_wait(entered, later)

    router_stage(1)
    mix_group(3)
    scale_and_send(2)
    send_sums(3)
    router_at = {4: 2, 7: 3, 9: 4, 11: 5, 13: 6}

    def pass_on(k):
        across_copy(k).wait_recv()
        passed_copy(k).start()

    for k in range(3, chunks):
        across_copy(k - 2).wait_send()
        scale_and_send(k)
        pass_on(k - 3)
        if k in router_at:
            router_stage(router_at[k])
    put_router()
    for g in range(len(groups)):
        for copy in sum_copies(g):
            copy.wait_send()
    for stage in stages:
        for copy in stage:
            copy.wait_send()
    across_copy(0).wait_send()
    for k in range(chunks - 3, chunks):
        pass_on(k)
    for k in range(chunks - 2, chunks):
        across_copy(k).wait_send()
    for k in range(chunks):
        beside_copy(k).wait_send()
        beside_copy(k).wait_recv()
    for k in range(chunks):
        passed_copy(k).wait_send()
        passed_copy(k).wait_recv()


def put_out(*refs):
    sems = refs[10]
    copies = [pltpu.make_async_copy(refs[n], refs[n + 5], sems.at[n]) for n in range(5)]
    for copy in copies:
        copy.start()
    for copy in copies:
        copy.wait()


def per_device(w_gate, avg_gate, w_up, avg_up, mix_share, router_weight, router_gain):
    _, rows, columns = w_gate.shape
    chunks = 2 * columns // LANES
    outs = pl.pallas_call(
        mix_and_send,
        out_shape=(
            pltpu.VMEM((4 * rows, columns), jnp.bfloat16),
            pltpu.VMEM((4 * rows, columns), jnp.bfloat16),
            pltpu.VMEM((1, columns), jnp.float32),
            pltpu.VMEM((1, columns), jnp.float32),
            pltpu.VMEM((64, 4 * rows), jnp.bfloat16),
        ),
        in_specs=[pl.BlockSpec(memory_space=pl.ANY)] * 7,
        out_specs=[pl.BlockSpec(memory_space=pltpu.VMEM)] * 5,
        scratch_shapes=[
            pltpu.VMEM((2, rows, columns), jnp.float32),
            pltpu.VMEM((2, rows, columns), jnp.float32),
            pltpu.VMEM((4, 1, chunks * LANES), jnp.float32),
            pltpu.VMEM((2, 4, 128, LANES), jnp.float32),
            pltpu.SMEM((1,), jnp.float32),
            pltpu.VMEM((2, 1, rows), jnp.float32),
            pltpu.SemaphoreType.DMA((3,)),
            pltpu.SemaphoreType.DMA((chunks, 2)),
            pltpu.SemaphoreType.DMA((4, 3)),
            pltpu.SemaphoreType.DMA((4, 3)),
        ]
        + [pltpu.SemaphoreType.DMA((chunks,))] * 6
        + [pltpu.SemaphoreType.DMA((11,))] * 2
        + [pltpu.SemaphoreType.REGULAR],
        compiler_params=pltpu.CompilerParams(
            collective_id=0, has_side_effects=True, vmem_limit_bytes=55 * 1024 * 1024
        ),
    )(
        w_gate, avg_gate, w_up, avg_up, mix_share,
        router_weight.reshape(1, rows), router_gain.reshape(1, rows),
    )
    gate, up, scale_gate, scale_up, router = pl.pallas_call(
        put_out,
        out_shape=[jax.ShapeDtypeStruct(o.shape, o.dtype) for o in outs],
        in_specs=[pl.BlockSpec(memory_space=pltpu.VMEM)] * 5,
        out_specs=[pl.BlockSpec(memory_space=pl.ANY)] * 5,
        scratch_shapes=[pltpu.SemaphoreType.DMA((5,))],
        compiler_params=pltpu.CompilerParams(vmem_limit_bytes=1024 * 1024),
    )(*outs)
    return gate[None], up[None], scale_gate, scale_up, router.T


def solution(mesh):
    return jax.shard_map(
        per_device,
        mesh=mesh,
        in_specs=(
            P("expert", "shard", None),
            P("expert", "shard", None),
            P("expert", "shard", None),
            P("expert", "shard", None),
            P("expert"),
            P("shard", "expert"),
            P("shard"),
        ),
        out_specs=(
            P("expert", None, None),
            P("expert", None, None),
            P("expert", None),
            P("expert", None),
            P(),
        ),
        check_vma=False,
    )
```

```python
import jax
import jax.numpy as jnp
from jax import lax
from jax.experimental import pallas as pl
from jax.experimental.pallas import tpu as pltpu
from jax.sharding import PartitionSpec as P

MESH = pl.DeviceIdType.MESH
LANES = 128
BLOCK = 64


PIECES = ((0, 0, 1), (0, 1, 2), (0, 3, 5), (1, 0, 4), (1, 4, 3), (1, 7, 1))
GROUPS = ((0,), (1,), (2,), (3, 4, 5))
TWICE = 128


def mix_and_send(
    w_gate, avg_gate, w_up, avg_up, mix_share, router_weight, router_gain,
    out_gate, out_up, out_scale_gate, out_scale_up, out_router,
    fresh, other, sums, router, share, factors,
    small_sem, load_sem, sum_send, sum_recv, across_send, across_recv, beside_send, beside_recv, passed_send, passed_recv,
    twice_send, twice_recv, router_send, router_recv, entered,
):
    rows, columns = fresh.shape[1], fresh.shape[2]
    pieces = len(PIECES)
    last = pieces - 1
    expert, shard = lax.axis_index("expert"), lax.axis_index("shard")
    far, core = shard // 2, shard % 2
    hi, y, x = expert // 16, (expert // 4) % 4, expert % 4
    across, beside, diagonal = (shard + 2) % 4, far * 2 + (1 - core), (1 - far) * 2 + (1 - core)
    peers = [(shard + d) % 4 for d in (1, 2, 3)]
    along_z = [(expert + 16 * d) % 64 for d in (1, 2, 3)]
    along_x = [hi * 16 + y * 4 + (x + d) % 4 for d in (1, 2, 3)]
    along_y = [hi * 16 + ((y + d) % 4) * 4 + x for d in (1, 2, 3)]

    def place(p):
        m, first, width = PIECES[p]
        return m, pl.ds(first * LANES, width * LANES)

    def load(p, which):
        m, cols = place(p)
        source = ((w_gate, avg_gate), (w_up, avg_up))[m][which]
        target = (fresh, other)[which]
        return pltpu.make_async_copy(source.at[0, :, cols], target.at[m, :, cols], load_sem.at[p, which])

    small = [
        pltpu.make_async_copy(mix_share, share, small_sem.at[0]),
        pltpu.make_async_copy(router_weight, factors.at[0], small_sem.at[1]),
        pltpu.make_async_copy(router_gain, factors.at[1], small_sem.at[2]),
    ]
    load(0, 0).start()
    load(0, 1).start()
    small[0].start()

    barrier = pltpu.get_barrier_semaphore()
    for p in peers:
        pl.semaphore_signal(barrier, inc=1, device_id=(expert, p), device_id_type=MESH)
    for p in range(1, pieces):
        load(p, 0).start()
        load(p, 1).start()
    router_peers = [(e, e > expert) for e in along_z + along_x + along_y]
    later = sum(after.astype(jnp.int32) for _, after in router_peers)
    for e, after in router_peers:

        @pl.when(after)
        def _():
            pl.semaphore_signal(barrier, inc=1, device_id=(e, shard), device_id_type=MESH)

    for copy in small[1:]:
        copy.start()
    small[0].wait()
    keep = share[0]
    rest = 1.0 - keep
    own = pl.multiple_of(shard * rows, rows)

    def blocks(p):
        m, first, width = PIECES[p]
        return m, [pl.ds((first + n) * LANES, LANES) for n in range(width)]

    def mix(p):
        load(p, 0).wait()
        load(p, 1).wait()
        m, parts = blocks(p)
        for cols in parts:

            def block(i, total):
                at = pl.ds(pl.multiple_of(i * BLOCK, BLOCK), BLOCK)
                value = keep * fresh[m, at, cols] + rest * other[m, at, cols]
                fresh[m, at, cols] = value
                return total + jnp.sum((value * value).reshape(BLOCK // 8, 8, LANES), axis=0)

            total = lax.fori_loop(0, rows // BLOCK, block, jnp.zeros((8, LANES), jnp.float32))
            sums[shard, :, pl.ds(m * columns + cols.start, LANES)] = jnp.sum(total, axis=0, keepdims=True)

    def sum_copies(g):
        m, first, _ = PIECES[GROUPS[g][0]]
        width = sum(PIECES[p][2] for p in GROUPS[g])
        part = sums.at[shard, :, pl.ds(m * columns + first * LANES, width * LANES)]
        return [
            pltpu.make_async_remote_copy(
                part, part, sum_send.at[g, d], sum_recv.at[g, d], device_id=(expert, peers[d]), device_id_type=MESH
            )
            for d in range(3)
        ]

    def mix_group(g):
        for p in GROUPS[g]:
            mix(p)

    def send_sums(g):
        for copy in sum_copies(g):
            copy.start()

    def wait_sums(g):
        for copy in sum_copies(g):
            copy.wait_recv()

    def moved(p, owner, start, count, device, send, recv):
        m, cols = place(p)
        piece = (out_gate, out_up)[m].at[pl.ds(pl.multiple_of(owner * rows + start, 128), count), cols]
        return pltpu.make_async_remote_copy(
            piece, piece, send, recv, device_id=(expert, device), device_id_type=MESH
        )

    def once(p):
        return rows - TWICE if p == last else rows

    def across_copy(p):
        return moved(p, shard, 0, once(p), across, across_send.at[p], across_recv.at[p])

    def beside_copy(p):
        return moved(p, shard, 0, rows, beside, beside_send.at[p], beside_recv.at[p])

    def passed_copy(p):
        return moved(p, across, 0, once(p), beside, passed_send.at[p], passed_recv.at[p])

    def twice_copies():
        return [
            moved(last, shard, rows - TWICE, TWICE, device, twice_send.at[n], twice_recv.at[n])
            for n, device in enumerate((across, diagonal))
        ]

    def scale_and_send(p):
        m, parts = blocks(p)
        target = (out_gate, out_up)[m]
        for cols in parts:
            at = pl.ds(m * columns + cols.start, LANES)
            scale = jnp.sqrt(sums[0, :, at] + sums[1, :, at] + sums[2, :, at] + sums[3, :, at])
            (out_scale_gate, out_scale_up)[m][:, cols] = scale
            inverse = 1.0 / scale

            def block(i, carry):
                at = pl.multiple_of(i * BLOCK, BLOCK)
                value = fresh[m, pl.ds(at, BLOCK), cols] * inverse
                target[pl.ds(pl.multiple_of(own + at, BLOCK), BLOCK), cols] = value.astype(jnp.bfloat16)
                return carry

            lax.fori_loop(0, rows // BLOCK, block, 0)
        across_copy(p).start()
        if p == last:
            for copy in twice_copies():
                copy.start()
        beside_copy(p).start()

    def pass_on(p):
        across_copy(p).wait_recv()
        passed_copy(p).start()

    def router_copy(piece, n, device):
        return pltpu.make_async_remote_copy(
            piece, piece, router_send.at[n], router_recv.at[n], device_id=device, device_id_type=MESH
        )

    tile = pl.multiple_of((expert % 16) * 8, 8)
    part = router.at[core, hi, pl.ds(pl.multiple_of(tile + far * 4, 4), 4)]
    mine = router.at[core, hi, pl.ds(tile, 8)]
    line = router.at[core, :, pl.ds(tile, 8)]
    plane = router.at[core, :, pl.ds(pl.multiple_of(y * 32, 32), 32)]
    stages = [
        [router_copy(part, 0, (expert, across))],
        [router_copy(mine, 1 + d, (along_z[d], shard)) for d in range(3)],
        [router_copy(line, 4 + d, (along_x[d], shard)) for d in range(3)],
        [router_copy(plane, 7 + d, (along_y[d], shard)) for d in range(3)],
        [router_copy(router.at[core], 10, (expert, beside))],
    ]

    def router_stage(n):
        if n > 0:
            for c in stages[n - 1]:
                c.wait_recv()
        if n < len(stages):
            for c in stages[n]:
                c.start()

    def put_router():
        for c in (0, 1):
            for f in (0, 1):
                for j in range(4):
                    at = (f * 2 + c) * 4 * LANES + j * LANES
                    for h in range(4):
                        piece = router[c, h, pl.ds(f * 4 + j, 16, stride=8), :]
                        out_router[h * 16 : (h + 1) * 16, at : at + LANES] = piece.astype(jnp.bfloat16)

    mix_group(0)
    pl.semaphore_wait(barrier, len(peers) + len(router_peers) - later)
    send_sums(0)
    for e, after in router_peers:

        @pl.when(jnp.logical_not(after))
        def _():
            pl.semaphore_signal(entered, inc=1, device_id=(e, shard), device_id_type=MESH)

    small[1].wait()
    small[2].wait()
    product = (factors[0] * factors[1]).astype(jnp.bfloat16).astype(jnp.float32)
    for j in range(4):
        router[core, hi, pl.ds(tile + far * 4 + j, 1)] = product[:, j * LANES : (j + 1) * LANES]
    mix_group(1)
    send_sums(1)
    router_stage(0)
    wait_sums(0)
    scale_and_send(0)
    mix_group(2)
    send_sums(2)
    wait_sums(1)
    scale_and_send(1)

    @pl.when(later > 0)
    def _():
        pl.semaphore_wait(entered, later)

    router_stage(1)
    mix_group(3)
    send_sums(3)
    wait_sums(2)
    scale_and_send(2)
    pass_on(0)
    wait_sums(3)
    scale_and_send(3)
    pass_on(1)
    router_stage(2)
    scale_and_send(4)
    scale_and_send(5)
    router_stage(3)
    router_stage(4)
    router_stage(5)
    put_router()
    pass_on(2)
    for g in range(len(GROUPS)):
        for copy in sum_copies(g):
            copy.wait_send()
    for stage in stages:
        for copy in stage:
            copy.wait_send()
    pass_on(3)
    for p in range(3):
        across_copy(p).wait_send()
        beside_copy(p).wait_send()
        beside_copy(p).wait_recv()
        passed_copy(p).wait_send()
        passed_copy(p).wait_recv()
    pass_on(4)
    for p in range(3, pieces):
        beside_copy(p).wait_send()
        beside_copy(p).wait_recv()
    pass_on(5)
    for p in range(3, pieces):
        across_copy(p).wait_send()
        passed_copy(p).wait_send()
        passed_copy(p).wait_recv()
    for copy in twice_copies():
        copy.wait_send()
        copy.wait_recv()


def put_out(*refs):
    sems = refs[10]
    copies = [pltpu.make_async_copy(refs[n], refs[n + 5], sems.at[n]) for n in range(5)]
    for copy in copies:
        copy.start()
    for copy in copies:
        copy.wait()


def per_device(w_gate, avg_gate, w_up, avg_up, mix_share, router_weight, router_gain):
    _, rows, columns = w_gate.shape
    pieces = len(PIECES)
    outs = pl.pallas_call(
        mix_and_send,
        out_shape=(
            pltpu.VMEM((4 * rows, columns), jnp.bfloat16),
            pltpu.VMEM((4 * rows, columns), jnp.bfloat16),
            pltpu.VMEM((1, columns), jnp.float32),
            pltpu.VMEM((1, columns), jnp.float32),
            pltpu.VMEM((64, 4 * rows), jnp.bfloat16),
        ),
        in_specs=[pl.BlockSpec(memory_space=pl.ANY)] * 7,
        out_specs=[pl.BlockSpec(memory_space=pltpu.VMEM)] * 5,
        scratch_shapes=[
            pltpu.VMEM((2, rows, columns), jnp.float32),
            pltpu.VMEM((2, rows, columns), jnp.float32),
            pltpu.VMEM((4, 1, 2 * columns), jnp.float32),
            pltpu.VMEM((2, 4, 128, LANES), jnp.float32),
            pltpu.SMEM((1,), jnp.float32),
            pltpu.VMEM((2, 1, rows), jnp.float32),
            pltpu.SemaphoreType.DMA((3,)),
            pltpu.SemaphoreType.DMA((pieces, 2)),
            pltpu.SemaphoreType.DMA((4, 3)),
            pltpu.SemaphoreType.DMA((4, 3)),
        ]
        + [pltpu.SemaphoreType.DMA((pieces,))] * 6
        + [pltpu.SemaphoreType.DMA((2,))] * 2
        + [pltpu.SemaphoreType.DMA((11,))] * 2
        + [pltpu.SemaphoreType.REGULAR],
        compiler_params=pltpu.CompilerParams(
            collective_id=0, has_side_effects=True, vmem_limit_bytes=55 * 1024 * 1024
        ),
    )(
        w_gate, avg_gate, w_up, avg_up, mix_share,
        router_weight.reshape(1, rows), router_gain.reshape(1, rows),
    )
    gate, up, scale_gate, scale_up, router = pl.pallas_call(
        put_out,
        out_shape=[jax.ShapeDtypeStruct(o.shape, o.dtype) for o in outs],
        in_specs=[pl.BlockSpec(memory_space=pltpu.VMEM)] * 5,
        out_specs=[pl.BlockSpec(memory_space=pl.ANY)] * 5,
        scratch_shapes=[pltpu.SemaphoreType.DMA((5,))],
        compiler_params=pltpu.CompilerParams(vmem_limit_bytes=1024 * 1024),
    )(*outs)
    return gate[None], up[None], scale_gate, scale_up, router.T


def solution(mesh):
    return jax.shard_map(
        per_device,
        mesh=mesh,
        in_specs=(
            P("expert", "shard", None),
            P("expert", "shard", None),
            P("expert", "shard", None),
            P("expert", "shard", None),
            P("expert"),
            P("shard", "expert"),
            P("shard"),
        ),
        out_specs=(
            P("expert", None, None),
            P("expert", None, None),
            P("expert", None),
            P("expert", None),
            P(),
        ),
        check_vma=False,
    )
```

```python
import jax
import jax.numpy as jnp
from jax import lax
from jax.experimental import pallas as pl
from jax.experimental.pallas import tpu as pltpu
from jax.sharding import PartitionSpec as P

MESH = pl.DeviceIdType.MESH
LANES = 128
BLOCK = 64


PIECES = ((0, 0, 1), (0, 1, 2), (0, 3, 5), (1, 0, 7), (1, 7, 1))
GROUPS = ((0,), (1,), (2,), (3, 4))
TWICE = 128
RAW = 128


def mix_and_send(
    w_gate, avg_gate, w_up, avg_up, mix_share, router_weight, router_gain,
    out_gate, out_up, out_scale_gate, out_scale_up, out_router,
    fresh, other, sums, router, share, factors, arrived,
    small_sem, load_sem, sum_send, sum_recv, across_send, across_recv, beside_send, beside_recv, passed_send, passed_recv,
    twice_send, twice_recv, raw_send, raw_recv, router_send, router_recv, entered,
):
    rows, columns = fresh.shape[1], fresh.shape[2]
    pieces = len(PIECES)
    last = pieces - 1
    expert, shard = lax.axis_index("expert"), lax.axis_index("shard")
    far, core = shard // 2, shard % 2
    hi, y, x = expert // 16, (expert // 4) % 4, expert % 4
    across, beside, diagonal = (shard + 2) % 4, far * 2 + (1 - core), (1 - far) * 2 + (1 - core)
    peers = [(shard + d) % 4 for d in (1, 2, 3)]
    along_z = [(expert + 16 * d) % 64 for d in (1, 2, 3)]
    along_x = [hi * 16 + y * 4 + (x + d) % 4 for d in (1, 2, 3)]
    along_y = [hi * 16 + ((y + d) % 4) * 4 + x for d in (1, 2, 3)]

    def place(p):
        m, first, width = PIECES[p]
        return m, pl.ds(first * LANES, width * LANES)

    def load(p, which):
        m, cols = place(p)
        source = ((w_gate, avg_gate), (w_up, avg_up))[m][which]
        target = (fresh, other)[which]
        return pltpu.make_async_copy(source.at[0, :, cols], target.at[m, :, cols], load_sem.at[p, which])

    small = [
        pltpu.make_async_copy(mix_share, share, small_sem.at[0]),
        pltpu.make_async_copy(router_weight, factors.at[0], small_sem.at[1]),
        pltpu.make_async_copy(router_gain, factors.at[1], small_sem.at[2]),
    ]
    barrier = pltpu.get_barrier_semaphore()
    for p in peers:
        pl.semaphore_signal(barrier, inc=1, device_id=(expert, p), device_id_type=MESH)
    load(0, 0).start()
    load(0, 1).start()
    small[0].start()
    for p in range(1, pieces):
        load(p, 0).start()
        load(p, 1).start()
    router_peers = [(e, e > expert) for e in along_z + along_x + along_y]
    later = sum(after.astype(jnp.int32) for _, after in router_peers)
    for e, after in router_peers:

        @pl.when(after)
        def _():
            pl.semaphore_signal(barrier, inc=1, device_id=(e, shard), device_id_type=MESH)

    for copy in small[1:]:
        copy.start()
    small[0].wait()
    keep = share[0]
    rest = 1.0 - keep
    own = pl.multiple_of(shard * rows, rows)

    def blocks(p):
        m, first, width = PIECES[p]
        return m, [pl.ds((first + n) * LANES, LANES) for n in range(width)]

    def mix(p):
        load(p, 0).wait()
        load(p, 1).wait()
        m, parts = blocks(p)
        for cols in parts:

            def block(i, total):
                at = pl.ds(pl.multiple_of(i * BLOCK, BLOCK), BLOCK)
                value = keep * fresh[m, at, cols] + rest * other[m, at, cols]
                fresh[m, at, cols] = value
                return total + jnp.sum((value * value).reshape(BLOCK // 8, 8, LANES), axis=0)

            total = lax.fori_loop(0, rows // BLOCK, block, jnp.zeros((8, LANES), jnp.float32), unroll=True)
            sums[shard, :, pl.ds(m * columns + cols.start, LANES)] = jnp.sum(total, axis=0, keepdims=True)

    def sum_copies(g):
        m, first, _ = PIECES[GROUPS[g][0]]
        width = sum(PIECES[p][2] for p in GROUPS[g])
        part = sums.at[shard, :, pl.ds(m * columns + first * LANES, width * LANES)]
        return [
            pltpu.make_async_remote_copy(
                part, part, sum_send.at[g, d], sum_recv.at[g, d], device_id=(expert, peers[d]), device_id_type=MESH
            )
            for d in range(3)
        ]

    def mix_group(g):
        for p in GROUPS[g]:
            mix(p)

    def send_sums(g):
        for copy in sum_copies(g):
            copy.start()

    def wait_sums(g):
        for copy in sum_copies(g):
            copy.wait_recv()

    def moved(p, owner, start, count, device, send, recv):
        m, cols = place(p)
        piece = (out_gate, out_up)[m].at[pl.ds(pl.multiple_of(owner * rows + start, 128), count), cols]
        return pltpu.make_async_remote_copy(
            piece, piece, send, recv, device_id=(expert, device), device_id_type=MESH
        )

    def across_copy(p):
        start, stop = RAW if p == 0 else 0, rows - TWICE if p == last else rows
        return moved(p, shard, start, stop - start, across, across_send.at[p], across_recv.at[p])

    def beside_copy(p):
        return moved(p, shard, 0, rows, beside, beside_send.at[p], beside_recv.at[p])

    def passed_copy(p):
        return moved(p, across, 0, rows - TWICE if p == last else rows, beside, passed_send.at[p], passed_recv.at[p])

    def twice_copies():
        return [
            moved(last, shard, rows - TWICE, TWICE, device, twice_send.at[n], twice_recv.at[n])
            for n, device in enumerate((across, diagonal))
        ]

    def raw_copy():
        return pltpu.make_async_remote_copy(
            fresh.at[0, pl.ds(0, RAW), pl.ds(0, LANES)], arrived, raw_send, raw_recv,
            device_id=(expert, across), device_id_type=MESH,
        )

    def scale_of(m, cols):
        at = pl.ds(m * columns + cols.start, LANES)
        return jnp.sqrt(sums[0, :, at] + sums[1, :, at] + sums[2, :, at] + sums[3, :, at])

    def scale_arrived():
        cols = pl.ds(0, LANES)
        raw_copy().wait_recv()
        value = arrived[...] * (1.0 / scale_of(0, cols))
        out_gate[pl.ds(pl.multiple_of(across * rows, rows), RAW), cols] = value.astype(jnp.bfloat16)

    def scale_and_send(p):
        m, parts = blocks(p)
        target = (out_gate, out_up)[m]
        for cols in parts:
            scale = scale_of(m, cols)
            (out_scale_gate, out_scale_up)[m][:, cols] = scale
            inverse = 1.0 / scale

            def block(i, carry):
                at = pl.multiple_of(i * BLOCK, BLOCK)
                value = fresh[m, pl.ds(at, BLOCK), cols] * inverse
                target[pl.ds(pl.multiple_of(own + at, BLOCK), BLOCK), cols] = value.astype(jnp.bfloat16)
                return carry

            lax.fori_loop(0, rows // BLOCK, block, 0, unroll=True)
        across_copy(p).start()
        if p == last:
            for copy in twice_copies():
                copy.start()
        beside_copy(p).start()

    def pass_on(p):
        across_copy(p).wait_recv()
        passed_copy(p).start()

    def router_copy(piece, n, device):
        return pltpu.make_async_remote_copy(
            piece, piece, router_send.at[n], router_recv.at[n], device_id=device, device_id_type=MESH
        )

    tile = pl.multiple_of((expert % 16) * 8, 8)
    part = router.at[core, hi, pl.ds(pl.multiple_of(tile + far * 4, 4), 4)]
    mine = router.at[core, hi, pl.ds(tile, 8)]
    line = router.at[core, :, pl.ds(tile, 8)]
    plane = router.at[core, :, pl.ds(pl.multiple_of(y * 32, 32), 32)]
    stages = [
        [router_copy(part, 0, (expert, across))],
        [router_copy(mine, 1 + d, (along_z[d], shard)) for d in range(3)],
        [router_copy(line, 4 + d, (along_x[d], shard)) for d in range(3)],
        [router_copy(plane, 7 + d, (along_y[d], shard)) for d in range(3)],
        [router_copy(router.at[core], 10, (expert, beside))],
    ]

    def router_stage(n):
        if n > 0:
            for c in stages[n - 1]:
                c.wait_recv()
        if n < len(stages):
            for c in stages[n]:
                c.start()

    def put_router():
        for c in (0, 1):
            for f in (0, 1):
                for j in range(4):
                    at = (f * 2 + c) * 4 * LANES + j * LANES
                    for h in range(4):
                        piece = router[c, h, pl.ds(f * 4 + j, 16, stride=8), :]
                        out_router[h * 16 : (h + 1) * 16, at : at + LANES] = piece.astype(jnp.bfloat16)

    mix_group(0)
    pl.semaphore_wait(barrier, len(peers) + len(router_peers) - later)
    send_sums(0)
    raw_copy().start()
    for e, after in router_peers:

        @pl.when(jnp.logical_not(after))
        def _():
            pl.semaphore_signal(entered, inc=1, device_id=(e, shard), device_id_type=MESH)

    small[1].wait()
    small[2].wait()
    product = (factors[0] * factors[1]).astype(jnp.bfloat16).astype(jnp.float32)
    for j in range(4):
        router[core, hi, pl.ds(tile + far * 4 + j, 1)] = product[:, j * LANES : (j + 1) * LANES]
    mix_group(1)
    send_sums(1)
    router_stage(0)
    mix_group(2)
    send_sums(2)
    wait_sums(0)
    scale_and_send(0)
    wait_sums(1)
    scale_and_send(1)

    @pl.when(later > 0)
    def _():
        pl.semaphore_wait(entered, later)

    router_stage(1)
    mix_group(3)
    send_sums(3)
    wait_sums(2)
    scale_and_send(2)
    scale_arrived()
    pass_on(0)
    wait_sums(3)
    scale_and_send(3)
    pass_on(1)
    router_stage(2)
    scale_and_send(4)
    router_stage(3)
    router_stage(4)
    router_stage(5)
    put_router()
    pass_on(2)
    for g in range(len(GROUPS)):
        for copy in sum_copies(g):
            copy.wait_send()
    for stage in stages:
        for copy in stage:
            copy.wait_send()
    pass_on(3)
    for p in range(3):
        across_copy(p).wait_send()
        beside_copy(p).wait_send()
        beside_copy(p).wait_recv()
        passed_copy(p).wait_send()
        passed_copy(p).wait_recv()
    for p in range(3, pieces):
        beside_copy(p).wait_send()
        beside_copy(p).wait_recv()
    pass_on(4)
    for p in range(3, pieces):
        across_copy(p).wait_send()
        passed_copy(p).wait_send()
        passed_copy(p).wait_recv()
    raw_copy().wait_send()
    for copy in twice_copies():
        copy.wait_send()
        copy.wait_recv()


def put_out(*refs):
    sems = refs[10]
    copies = [pltpu.make_async_copy(refs[n], refs[n + 5], sems.at[n]) for n in range(5)]
    for copy in copies:
        copy.start()
    for copy in copies:
        copy.wait()


def per_device(w_gate, avg_gate, w_up, avg_up, mix_share, router_weight, router_gain):
    _, rows, columns = w_gate.shape
    pieces = len(PIECES)
    outs = pl.pallas_call(
        mix_and_send,
        out_shape=(
            pltpu.VMEM((4 * rows, columns), jnp.bfloat16),
            pltpu.VMEM((4 * rows, columns), jnp.bfloat16),
            pltpu.VMEM((1, columns), jnp.float32),
            pltpu.VMEM((1, columns), jnp.float32),
            pltpu.VMEM((64, 4 * rows), jnp.bfloat16),
        ),
        in_specs=[pl.BlockSpec(memory_space=pl.ANY)] * 7,
        out_specs=[pl.BlockSpec(memory_space=pltpu.VMEM)] * 5,
        scratch_shapes=[
            pltpu.VMEM((2, rows, columns), jnp.float32),
            pltpu.VMEM((2, rows, columns), jnp.float32),
            pltpu.VMEM((4, 1, 2 * columns), jnp.float32),
            pltpu.VMEM((2, 4, 128, LANES), jnp.float32),
            pltpu.SMEM((1,), jnp.float32),
            pltpu.VMEM((2, 1, rows), jnp.float32),
            pltpu.VMEM((RAW, LANES), jnp.float32),
            pltpu.SemaphoreType.DMA((3,)),
            pltpu.SemaphoreType.DMA((pieces, 2)),
            pltpu.SemaphoreType.DMA((4, 3)),
            pltpu.SemaphoreType.DMA((4, 3)),
        ]
        + [pltpu.SemaphoreType.DMA((pieces,))] * 6
        + [pltpu.SemaphoreType.DMA((2,))] * 2
        + [pltpu.SemaphoreType.DMA(())] * 2
        + [pltpu.SemaphoreType.DMA((11,))] * 2
        + [pltpu.SemaphoreType.REGULAR],
        compiler_params=pltpu.CompilerParams(
            collective_id=0, has_side_effects=True, vmem_limit_bytes=55 * 1024 * 1024
        ),
    )(
        w_gate, avg_gate, w_up, avg_up, mix_share,
        router_weight.reshape(1, rows), router_gain.reshape(1, rows),
    )
    gate, up, scale_gate, scale_up, router = pl.pallas_call(
        put_out,
        out_shape=[jax.ShapeDtypeStruct(o.shape, o.dtype) for o in outs],
        in_specs=[pl.BlockSpec(memory_space=pltpu.VMEM)] * 5,
        out_specs=[pl.BlockSpec(memory_space=pl.ANY)] * 5,
        scratch_shapes=[pltpu.SemaphoreType.DMA((5,))],
        compiler_params=pltpu.CompilerParams(vmem_limit_bytes=1024 * 1024),
    )(*outs)
    return gate[None], up[None], scale_gate, scale_up, router.T


def solution(mesh):
    return jax.shard_map(
        per_device,
        mesh=mesh,
        in_specs=(
            P("expert", "shard", None),
            P("expert", "shard", None),
            P("expert", "shard", None),
            P("expert", "shard", None),
            P("expert"),
            P("shard", "expert"),
            P("shard"),
        ),
        out_specs=(
            P("expert", None, None),
            P("expert", None, None),
            P("expert", None),
            P("expert", None),
            P(),
        ),
        check_vma=False,
    )
```

```python
import jax
import jax.numpy as jnp
from jax import lax
from jax.experimental import pallas as pl
from jax.experimental.pallas import tpu as pltpu
from jax.sharding import PartitionSpec as P

MESH = pl.DeviceIdType.MESH
LANES = 128
BLOCK = 64


PIECES = ((0, 0, 1), (0, 1, 2), (0, 3, 5), (1, 0, 7), (1, 7, 1))
GROUPS = ((0,), (1,), (2,), (3, 4))
TWICE = 128


def mix_and_send(
    w_gate, avg_gate, w_up, avg_up, mix_share, router_weight, router_gain,
    out_gate, out_up, out_scale_gate, out_scale_up, out_router,
    fresh, other, sums, router, share, factors,
    small_sem, load_sem, sum_send, sum_recv, across_send, across_recv, beside_send, beside_recv, passed_send, passed_recv,
    twice_send, twice_recv, router_send, router_recv, entered,
):
    rows, columns = fresh.shape[1], fresh.shape[2]
    pieces = len(PIECES)
    last = pieces - 1
    expert, shard = lax.axis_index("expert"), lax.axis_index("shard")
    far, core = shard // 2, shard % 2
    hi, y, x = expert // 16, (expert // 4) % 4, expert % 4
    across, beside, diagonal = (shard + 2) % 4, far * 2 + (1 - core), (1 - far) * 2 + (1 - core)
    peers = [(shard + d) % 4 for d in (1, 2, 3)]
    along_z = [(expert + 16 * d) % 64 for d in (1, 2, 3)]
    along_x = [hi * 16 + y * 4 + (x + d) % 4 for d in (1, 2, 3)]
    along_y = [hi * 16 + ((y + d) % 4) * 4 + x for d in (1, 2, 3)]

    def place(p):
        m, first, width = PIECES[p]
        return m, pl.ds(first * LANES, width * LANES)

    def load(p, which):
        m, cols = place(p)
        source = ((w_gate, avg_gate), (w_up, avg_up))[m][which]
        target = (fresh, other)[which]
        return pltpu.make_async_copy(source.at[0, :, cols], target.at[m, :, cols], load_sem.at[p, which])

    small = [
        pltpu.make_async_copy(mix_share, share, small_sem.at[0]),
        pltpu.make_async_copy(router_weight, factors.at[0], small_sem.at[1]),
        pltpu.make_async_copy(router_gain, factors.at[1], small_sem.at[2]),
    ]
    barrier = pltpu.get_barrier_semaphore()
    for p in peers:
        pl.semaphore_signal(barrier, inc=1, device_id=(expert, p), device_id_type=MESH)
    load(0, 0).start()
    load(0, 1).start()
    small[0].start()
    for p in range(1, pieces):
        load(p, 0).start()
        load(p, 1).start()
    router_peers = [(e, e > expert) for e in along_z + along_x + along_y]
    later = sum(after.astype(jnp.int32) for _, after in router_peers)
    for e, after in router_peers:

        @pl.when(after)
        def _():
            pl.semaphore_signal(barrier, inc=1, device_id=(e, shard), device_id_type=MESH)

    for copy in small[1:]:
        copy.start()
    small[0].wait()
    keep = share[0]
    rest = 1.0 - keep
    own = pl.multiple_of(shard * rows, rows)

    def blocks(p):
        m, first, width = PIECES[p]
        return m, [pl.ds((first + n) * LANES, LANES) for n in range(width)]

    def mix(p):
        load(p, 0).wait()
        load(p, 1).wait()
        m, parts = blocks(p)
        for cols in parts:

            def block(i, total):
                at = pl.ds(pl.multiple_of(i * BLOCK, BLOCK), BLOCK)
                value = keep * fresh[m, at, cols] + rest * other[m, at, cols]
                fresh[m, at, cols] = value
                return total + jnp.sum((value * value).reshape(BLOCK // 8, 8, LANES), axis=0)

            total = lax.fori_loop(0, rows // BLOCK, block, jnp.zeros((8, LANES), jnp.float32), unroll=True)
            sums[shard, :, pl.ds(m * columns + cols.start, LANES)] = jnp.sum(total, axis=0, keepdims=True)

    def sum_copies(g):
        m, first, _ = PIECES[GROUPS[g][0]]
        width = sum(PIECES[p][2] for p in GROUPS[g])
        part = sums.at[shard, :, pl.ds(m * columns + first * LANES, width * LANES)]
        return [
            pltpu.make_async_remote_copy(
                part, part, sum_send.at[g, d], sum_recv.at[g, d], device_id=(expert, peers[d]), device_id_type=MESH
            )
            for d in range(3)
        ]

    def mix_group(g):
        for p in GROUPS[g]:
            mix(p)

    def send_sums(g):
        for copy in sum_copies(g):
            copy.start()

    def wait_sums(g):
        for copy in sum_copies(g):
            copy.wait_recv()

    def moved(p, owner, start, count, device, send, recv):
        m, cols = place(p)
        piece = (out_gate, out_up)[m].at[pl.ds(pl.multiple_of(owner * rows + start, 128), count), cols]
        return pltpu.make_async_remote_copy(
            piece, piece, send, recv, device_id=(expert, device), device_id_type=MESH
        )

    def once(p):
        return rows - TWICE if p == last else rows

    def across_copy(p):
        return moved(p, shard, 0, once(p), across, across_send.at[p], across_recv.at[p])

    def beside_copy(p):
        return moved(p, shard, 0, rows, beside, beside_send.at[p], beside_recv.at[p])

    def passed_copy(p):
        return moved(p, across, 0, once(p), beside, passed_send.at[p], passed_recv.at[p])

    def twice_copies():
        return [
            moved(last, shard, rows - TWICE, TWICE, device, twice_send.at[n], twice_recv.at[n])
            for n, device in enumerate((across, diagonal))
        ]

    def scale_and_send(p):
        m, parts = blocks(p)
        target = (out_gate, out_up)[m]
        for cols in parts:
            at = pl.ds(m * columns + cols.start, LANES)
            scale = jnp.sqrt(sums[0, :, at] + sums[1, :, at] + sums[2, :, at] + sums[3, :, at])
            (out_scale_gate, out_scale_up)[m][:, cols] = scale
            inverse = 1.0 / scale

            def block(i, carry):
                at = pl.multiple_of(i * BLOCK, BLOCK)
                value = fresh[m, pl.ds(at, BLOCK), cols] * inverse
                target[pl.ds(pl.multiple_of(own + at, BLOCK), BLOCK), cols] = value.astype(jnp.bfloat16)
                return carry

            lax.fori_loop(0, rows // BLOCK, block, 0, unroll=True)
        across_copy(p).start()
        if p == last:
            for copy in twice_copies():
                copy.start()
        beside_copy(p).start()

    def pass_on(p):
        across_copy(p).wait_recv()
        passed_copy(p).start()

    def router_copy(piece, n, device):
        return pltpu.make_async_remote_copy(
            piece, piece, router_send.at[n], router_recv.at[n], device_id=device, device_id_type=MESH
        )

    tile = pl.multiple_of((expert % 16) * 8, 8)
    part = router.at[core, hi, pl.ds(pl.multiple_of(tile + far * 4, 4), 4)]
    mine = router.at[core, hi, pl.ds(tile, 8)]
    line = router.at[core, :, pl.ds(tile, 8)]
    plane = router.at[core, :, pl.ds(pl.multiple_of(y * 32, 32), 32)]
    stages = [
        [router_copy(part, 0, (expert, across))],
        [router_copy(mine, 1 + d, (along_z[d], shard)) for d in range(3)],
        [router_copy(line, 4 + d, (along_x[d], shard)) for d in range(3)],
        [router_copy(plane, 7 + d, (along_y[d], shard)) for d in range(3)],
        [router_copy(router.at[core], 10, (expert, beside))],
    ]

    def router_stage(n):
        if n > 0:
            for c in stages[n - 1]:
                c.wait_recv()
        if n < len(stages):
            for c in stages[n]:
                c.start()

    def put_router():
        for c in (0, 1):
            for f in (0, 1):
                for j in range(4):
                    at = (f * 2 + c) * 4 * LANES + j * LANES
                    for h in range(4):
                        piece = router[c, h, pl.ds(f * 4 + j, 16, stride=8), :]
                        out_router[h * 16 : (h + 1) * 16, at : at + LANES] = piece.astype(jnp.bfloat16)

    mix_group(0)
    pl.semaphore_wait(barrier, len(peers) + len(router_peers) - later)
    send_sums(0)
    for e, after in router_peers:

        @pl.when(jnp.logical_not(after))
        def _():
            pl.semaphore_signal(entered, inc=1, device_id=(e, shard), device_id_type=MESH)

    small[1].wait()
    small[2].wait()
    product = (factors[0] * factors[1]).astype(jnp.bfloat16).astype(jnp.float32)
    for j in range(4):
        router[core, hi, pl.ds(tile + far * 4 + j, 1)] = product[:, j * LANES : (j + 1) * LANES]
    mix_group(1)
    send_sums(1)
    router_stage(0)
    mix_group(2)
    send_sums(2)
    wait_sums(0)
    scale_and_send(0)
    wait_sums(1)
    scale_and_send(1)

    @pl.when(later > 0)
    def _():
        pl.semaphore_wait(entered, later)

    router_stage(1)
    mix_group(3)
    send_sums(3)
    wait_sums(2)
    scale_and_send(2)
    pass_on(0)
    wait_sums(3)
    scale_and_send(3)
    pass_on(1)
    router_stage(2)
    scale_and_send(4)
    router_stage(3)
    router_stage(4)
    router_stage(5)
    put_router()
    pass_on(2)
    for g in range(len(GROUPS)):
        for copy in sum_copies(g):
            copy.wait_send()
    for stage in stages:
        for copy in stage:
            copy.wait_send()
    pass_on(3)
    for p in range(3):
        across_copy(p).wait_send()
        beside_copy(p).wait_send()
        beside_copy(p).wait_recv()
        passed_copy(p).wait_send()
        passed_copy(p).wait_recv()
    for p in range(3, pieces):
        beside_copy(p).wait_send()
        beside_copy(p).wait_recv()
    pass_on(4)
    for p in range(3, pieces):
        across_copy(p).wait_send()
        passed_copy(p).wait_send()
        passed_copy(p).wait_recv()
    for copy in twice_copies():
        copy.wait_send()
        copy.wait_recv()


def put_out(*refs):
    sems = refs[10]
    copies = [pltpu.make_async_copy(refs[n], refs[n + 5], sems.at[n]) for n in range(5)]
    for copy in copies:
        copy.start()
    for copy in copies:
        copy.wait()


def per_device(w_gate, avg_gate, w_up, avg_up, mix_share, router_weight, router_gain):
    _, rows, columns = w_gate.shape
    pieces = len(PIECES)
    outs = pl.pallas_call(
        mix_and_send,
        out_shape=(
            pltpu.VMEM((4 * rows, columns), jnp.bfloat16),
            pltpu.VMEM((4 * rows, columns), jnp.bfloat16),
            pltpu.VMEM((1, columns), jnp.float32),
            pltpu.VMEM((1, columns), jnp.float32),
            pltpu.VMEM((64, 4 * rows), jnp.bfloat16),
        ),
        in_specs=[pl.BlockSpec(memory_space=pl.ANY)] * 7,
        out_specs=[pl.BlockSpec(memory_space=pltpu.VMEM)] * 5,
        scratch_shapes=[
            pltpu.VMEM((2, rows, columns), jnp.float32),
            pltpu.VMEM((2, rows, columns), jnp.float32),
            pltpu.VMEM((4, 1, 2 * columns), jnp.float32),
            pltpu.VMEM((2, 4, 128, LANES), jnp.float32),
            pltpu.SMEM((1,), jnp.float32),
            pltpu.VMEM((2, 1, rows), jnp.float32),
            pltpu.SemaphoreType.DMA((3,)),
            pltpu.SemaphoreType.DMA((pieces, 2)),
            pltpu.SemaphoreType.DMA((4, 3)),
            pltpu.SemaphoreType.DMA((4, 3)),
        ]
        + [pltpu.SemaphoreType.DMA((pieces,))] * 6
        + [pltpu.SemaphoreType.DMA((2,))] * 2
        + [pltpu.SemaphoreType.DMA((11,))] * 2
        + [pltpu.SemaphoreType.REGULAR],
        compiler_params=pltpu.CompilerParams(
            collective_id=0, has_side_effects=True, vmem_limit_bytes=55 * 1024 * 1024
        ),
    )(
        w_gate, avg_gate, w_up, avg_up, mix_share,
        router_weight.reshape(1, rows), router_gain.reshape(1, rows),
    )
    gate, up, scale_gate, scale_up, router = pl.pallas_call(
        put_out,
        out_shape=[jax.ShapeDtypeStruct(o.shape, o.dtype) for o in outs],
        in_specs=[pl.BlockSpec(memory_space=pltpu.VMEM)] * 5,
        out_specs=[pl.BlockSpec(memory_space=pl.ANY)] * 5,
        scratch_shapes=[pltpu.SemaphoreType.DMA((5,))],
        compiler_params=pltpu.CompilerParams(vmem_limit_bytes=1024 * 1024),
    )(*outs)
    return gate[None], up[None], scale_gate, scale_up, router.T


def solution(mesh):
    return jax.shard_map(
        per_device,
        mesh=mesh,
        in_specs=(
            P("expert", "shard", None),
            P("expert", "shard", None),
            P("expert", "shard", None),
            P("expert", "shard", None),
            P("expert"),
            P("shard", "expert"),
            P("shard"),
        ),
        out_specs=(
            P("expert", None, None),
            P("expert", None, None),
            P("expert", None),
            P("expert", None),
            P(),
        ),
        check_vma=False,
    )
```
